32 devices in a mesh: dp: 2 (over z, core), tp: 16 (over x, y).
Axes of the slice: x: 4, y: 4, z: 1, core: 2. Of those that a mesh axis runs over, the one named last changes fastest.
The devices are a block of a 4x4x8 slice.
Arguments:
- x: bfloat16 [4096, 1024], P('dp'), parts along dimension 0
- gain: bfloat16 [1024], replicated
- wq: bfloat16 [1024, 16384], P(None, 'tp')
- wk: bfloat16 [1024, 16384], P(None, 'tp')
- wv: bfloat16 [1024, 16384], P(None, 'tp')
- wo: bfloat16 [16384, 1024], P('tp')
Outputs:
- output: bfloat16 [4096, 1024], P('dp'), parts along dimension 0
There are 2 independent parts. The reference program is written for one: setup_inputs(seed, part) draws one part's arguments, and reference() takes and returns one part's arrays. A program takes and returns all parts, laid end to end along the dimension named above; an argument that names none is the same for every part.
All inputs are finite; a program needn't handle non-finite values.
Results may differ from the reference program's by a relative error of at most 0.012.
Values are sent between devices in bfloat16 or wider.
A program may use at most 768 MiB of HBM per device.

```python
import jax
import jax.numpy as jnp
from jax import lax

ROWS = 2048
D = 1024
HEADS = 128
KV_HEADS = 128
HEAD = 128
THETA = 10000


def setup_inputs(seed: int = 0, part: int = 0) -> dict:
    kx, kn, kq, kk, kv, ko = jax.random.split(jax.random.key(seed), 6)

    def weights(key, rows, columns):
        return jax.random.normal(key, (rows, columns), jnp.float32) * rows**-0.5

    drawn = {
        "x": jax.random.normal(jax.random.fold_in(kx, part), (ROWS, D), jnp.float32),
        "gain": 1 + 0.1 * jax.random.normal(kn, (D,), jnp.float32),
        "wq": 2 * weights(kq, D, HEADS * HEAD),
        "wk": 2 * weights(kk, D, KV_HEADS * HEAD),
        "wv": 4 * weights(kv, D, KV_HEADS * HEAD),
        "wo": weights(ko, HEADS * HEAD, D),
    }
    return {k: v.astype(jnp.bfloat16) for k, v in drawn.items()}


def normed(x, gain):
    wide = x.astype(jnp.float32)
    scale = lax.rsqrt(jnp.mean(wide * wide, -1, keepdims=True) + 1e-6)
    return (wide * scale * gain.astype(jnp.float32)).astype(jnp.bfloat16)


def turned(t, place, theta):
    half = t.shape[-1] // 2
    angle = place.astype(jnp.float32)[:, None] * theta ** (-jnp.arange(half, dtype=jnp.float32) / half)
    cos, sin = jnp.cos(angle)[:, None], jnp.sin(angle)[:, None]
    a, b = t[..., :half].astype(jnp.float32), t[..., half:].astype(jnp.float32)
    return jnp.concatenate([a * cos - b * sin, b * cos + a * sin], -1).astype(jnp.bfloat16)


def matmul(a, w):
    return jnp.dot(a, w, preferred_element_type=jnp.float32).astype(jnp.bfloat16)


def einsum(form, a, b):
    return jnp.einsum(form, a.astype(jnp.float32), b.astype(jnp.float32))


def attention(q, k, v):
    scores = einsum("tgsd,ugd->gstu", q, k) * q.shape[-1] ** -0.5
    token = jnp.arange(q.shape[0])
    scores = jnp.where(token[:, None] >= token, scores, -jnp.inf)
    weights = jax.nn.softmax(scores, -1).astype(jnp.bfloat16)
    return einsum("gstu,ugd->tgsd", weights, v).astype(jnp.bfloat16)


def reference(x, gain, wq, wk, wv, wo):
    a, place = normed(x, gain), jnp.arange(ROWS)
    q = turned(matmul(a, wq).reshape(ROWS, HEADS, HEAD), place, THETA).reshape(ROWS, KV_HEADS, -1, HEAD)
    k = turned(matmul(a, wk).reshape(ROWS, KV_HEADS, HEAD), place, THETA)
    v = matmul(a, wv).reshape(ROWS, KV_HEADS, HEAD)
    seen = attention(q, k, v).reshape(ROWS, HEADS * HEAD)
    return (x.astype(jnp.float32) + jnp.dot(seen, wo, preferred_element_type=jnp.float32)).astype(jnp.bfloat16)
```

```python
import functools
import math

import jax
import jax.numpy as jnp
import numpy as np
from jax import lax
from jax.experimental import pallas as pl
from jax.experimental.pallas import tpu as pltpu
from jax.sharding import PartitionSpec as P

HEAD = 128
THETA = 10000
LOG2E = 1.4426950408889634
EXP = HEAD**-0.5 * LOG2E
BLOCK = 512
VMEM = 63 * 2**20


def _dot(a, b, ca, cb):
    return lax.dot_general(a, b, (((ca,), (cb,)), ((), ())), preferred_element_type=jnp.float32)


def _tables(rows):
    half = HEAD // 2
    power = (np.float32(THETA) ** (-np.arange(half, dtype=np.float32) / np.float32(half))).astype(np.float32)
    angle = (np.arange(rows, dtype=np.float32)[:, None] * power).astype(np.float64)
    cos, sin = np.cos(angle).astype(np.float32), np.sin(angle).astype(np.float32)
    return np.concatenate([cos, cos], 1), np.concatenate([-sin, sin], 1)


def _kernel(side, x_ref, gain_ref, cos_ref, sin_ref, wq_ref, wk_ref, wv_ref, wo_ref, y_ref,
            a_s, q_s, k_s, vt_s, o_s, top_s, sum_s, mix_s, term_s, part_s,
            s1, s2, s3, s4, r1, r2, r3, r4, send_sem, recv_sem):
    rows, width = x_ref.shape
    bq = a_s.shape[0]
    blocks = rows // bq
    heads = wq_ref.shape[1] // HEAD
    quarter, piece = bq // side, bq // side**2
    wide = width // 2
    thin = wide // 2

    me = lax.axis_index("tp")
    here = (lax.div(me, side), lax.rem(me, side))

    def at(axis, n):
        moved = lax.rem(here[axis] + n + side, side)
        return moved * side + here[1] if axis == 0 else here[0] * side + moved

    near = [(at(axis, 1), at(axis, -1)) for axis in (0, 1)]
    barrier = pltpu.get_barrier_semaphore()
    for pair in near:
        for device in pair:
            pl.semaphore_signal(barrier, inc=1, device_id={"tp": device}, device_id_type=pl.DeviceIdType.MESH)
    pl.semaphore_wait(barrier, 4)


    def remote(c, half, n, way, src, dst, device):
        return pltpu.make_async_remote_copy(
            src_ref=src, dst_ref=dst, send_sem=send_sem.at[c, half, n, way], recv_sem=recv_sem.at[c, half, n, way],
            device_id={"tp": device}, device_id_type=pl.DeviceIdType.MESH)

    def step(c, n, action):
        for half in (0, 1):
            first, second = half, 1 - half
            p1, p2 = here[first], here[second]
            left, right, both = (pl.ds(half * wide + f * thin, w) for f, w in ((0, thin), (1, thin), (0, wide)))
            base = c * bq

            def rows1(k):
                return pl.ds(pl.multiple_of(base + lax.rem(p1 + k, side) * quarter, quarter), quarter)

            def rows2(k):
                return pl.ds(pl.multiple_of(base + p1 * quarter + lax.rem(p2 + k, side) * piece, piece), piece)

            for way in (0, 1):
                device = near[first if n in (0, 1, 6, 7) else second][way]
                if n < 4:
                    s, r = ((s1, r1), (s2, r2), (s3, r3), (s4, r4))[n]
                    src, dst = s.at[c, half, way], r.at[c, half, way]
                else:
                    if n == 4:
                        where = (rows2(0), both)
                    elif n == 5:
                        where = (rows2(side - 1), left) if way == 0 else (rows2(1), right)
                    elif n == 6:
                        where = (rows1(0), both)
                    else:
                        where = (rows1(side - 1), left) if way == 0 else (rows1(1), right)
                    src = dst = y_ref.at[where]
                action(remote(c, half, n, way, src, dst, device))

    def prepare(c, n):
        for half in (0, 1):
            first, second = half, 1 - half
            p1, p2 = here[first], here[second]
            lo = half * wide

            def rows1(k):
                return pl.ds(pl.multiple_of(lax.rem(p1 + k, side) * quarter, quarter), quarter)

            def rows2(k):
                return pl.ds(pl.multiple_of(lax.rem(p2 + k, side) * piece, piece), piece)

            if n == 0:
                far = rows1(side // 2)
                s1[c, half, 0] = term_s[far, lo : lo + thin].astype(jnp.bfloat16)
                s1[c, half, 1] = term_s[far, lo + thin : lo + wide].astype(jnp.bfloat16)
            elif n == 1:
                up, down = rows1(1), rows1(side - 1)
                s2[c, half, 0, :, :thin] = (term_s[up, lo : lo + thin] + r1[c, half, 0].astype(jnp.float32)).astype(jnp.bfloat16)
                s2[c, half, 0, :, thin:] = term_s[up, lo + thin : lo + wide].astype(jnp.bfloat16)
                s2[c, half, 1, :, :thin] = term_s[down, lo : lo + thin].astype(jnp.bfloat16)
                s2[c, half, 1, :, thin:] = (term_s[down, lo + thin : lo + wide] + r1[c, half, 1].astype(jnp.float32)).astype(jnp.bfloat16)
            elif n == 2:
                part_s[half] = (term_s[rows1(0), lo : lo + wide] + r2[c, half, 0].astype(jnp.float32)) + r2[c, half, 1].astype(jnp.float32)
                far = rows2(side // 2)
                s3[c, half, 0] = part_s[half, far, :thin].astype(jnp.bfloat16)
                s3[c, half, 1] = part_s[half, far, thin:].astype(jnp.bfloat16)
            elif n == 3:
                up, down = rows2(1), rows2(side - 1)
                s4[c, half, 0, :, :thin] = (part_s[half, up, :thin] + r3[c, half, 0].astype(jnp.float32)).astype(jnp.bfloat16)
                s4[c, half, 0, :, thin:] = part_s[half, up, thin:].astype(jnp.bfloat16)
                s4[c, half, 1, :, :thin] = part_s[half, down, :thin].astype(jnp.bfloat16)
                s4[c, half, 1, :, thin:] = (part_s[half, down, thin:] + r3[c, half, 1].astype(jnp.float32)).astype(jnp.bfloat16)
            elif n == 4:
                own = (part_s[half, rows2(0), :] + r4[c, half, 0].astype(jnp.float32)) + r4[c, half, 1].astype(jnp.float32)
                where = pl.ds(pl.multiple_of(c * bq + p1 * quarter + p2 * piece, piece), piece)
                y_ref[where, lo : lo + wide] = (x_ref[where, lo : lo + wide].astype(jnp.float32) + own).astype(jnp.bfloat16)

    def advance(c, n):
        @pl.when((c >= 0) & (c < blocks))
        def _():
            if n > 0:
                step(c, n - 1, lambda copy: copy.wait_recv())
            prepare(c, n)
            step(c, n, lambda copy: copy.start())

    slots = 4

    def slot(i, k):
        for d in range(8 // slots):
            advance(i - 1 - d, k + slots * d)


    def project(i):
        mine = pl.ds(pl.multiple_of(i * bq, bq), bq)
        xw = x_ref[mine, :].astype(jnp.float32)
        scale = lax.rsqrt(jnp.mean(xw * xw, -1, keepdims=True) + 1e-6)
        a_s[...] = (xw * scale * gain_ref[...].astype(jnp.float32)).astype(jnp.bfloat16)
        cos, sin = cos_ref[mine, :], sin_ref[mine, :]

        def turned(t):
            t = t.astype(jnp.bfloat16).astype(jnp.float32)
            return (t * cos + pltpu.roll(t, HEAD // 2, 1) * sin).astype(jnp.bfloat16)

        two = 2 * HEAD
        for at_ in range(0, heads * HEAD, two):
            q = _dot(a_s[...], wq_ref[:, at_ : at_ + two], 1, 0)
            k = _dot(a_s[...], wk_ref[:, at_ : at_ + two], 1, 0)
            v = _dot(a_s[...], wv_ref[:, at_ : at_ + two], 1, 0)
            for b in (0, HEAD):
                q_s[:, at_ + b : at_ + b + HEAD] = turned(q[:, b : b + HEAD])
                k_s[mine, at_ + b : at_ + b + HEAD] = turned(k[:, b : b + HEAD])
            vt_s[at_ : at_ + two, mine] = v.astype(jnp.bfloat16).T
        top_s[...] = jnp.full(top_s.shape, -jnp.inf, jnp.float32)
        sum_s[...] = jnp.zeros(sum_s.shape, jnp.float32)
        mix_s[...] = jnp.zeros(mix_s.shape, jnp.float32)

    def tile(j, masked):
        keys = pl.ds(pl.multiple_of(j * bq, bq), bq)
        scores, weights, keeps = {}, {}, {}
        if masked:
            ok = lax.broadcasted_iota(jnp.int32, (bq, bq), 1) >= lax.broadcasted_iota(jnp.int32, (bq, bq), 0)

        def score(h):
            cols = slice(h * HEAD, (h + 1) * HEAD)
            scores[h] = _dot(k_s[keys, cols], q_s[:, cols], 1, 1)

        def weigh(h):
            s = jnp.where(ok, scores.pop(h), -jnp.inf) if masked else scores.pop(h)
            old = top_s[h : h + 1, :]
            top = jnp.maximum(old, s.max(axis=0, keepdims=True))
            w = jnp.exp2((s - top) * EXP)
            keep = jnp.exp2((old - top) * EXP)
            top_s[h : h + 1, :] = top
            sum_s[h] = sum_s[h] * keep + w.reshape(bq // 8, 8, bq).sum(axis=0)
            weights[h], keeps[h] = w.astype(jnp.bfloat16), keep

        def mix(h):
            mix_s[h] = mix_s[h] * keeps.pop(h) + _dot(vt_s[h * HEAD : (h + 1) * HEAD, keys], weights.pop(h), 1, 0)

        score(0)
        for h in range(heads):
            if h + 1 < heads:
                score(h + 1)
            weigh(h)
            if h > 0:
                mix(h - 1)
        mix(heads - 1)

    def finish():
        for h in range(heads):
            total = sum_s[h].sum(axis=0, keepdims=True)
            o_s[:, h * HEAD : (h + 1) * HEAD] = (mix_s[h] * (1 / total)).astype(jnp.bfloat16).T
        for n in range(0, width, 2 * HEAD):
            term_s[:, n : n + 2 * HEAD] = _dot(o_s[...], wo_ref[:, n : n + 2 * HEAD], 1, 0)

    def block(i, _):
        busy = i < blocks
        slot(i, 0)

        @pl.when(busy)
        def _():
            project(i)

        slot(i, 1)
        middle = lax.div(i, 2)

        @pl.when(busy)
        def _():
            lax.fori_loop(0, middle, lambda j, _: tile(j, False), None)

        slot(i, 2)

        @pl.when(busy)
        def _():
            lax.fori_loop(middle, i, lambda j, _: tile(j, False), None)
            tile(i, True)

        slot(i, 3)

        @pl.when(busy)
        def _():
            finish()

    lax.fori_loop(0, blocks + 8 // slots, block, None)

    def drain(c, _):
        step(c, 7, lambda copy: copy.wait_recv())
        for n in range(8):
            step(c, n, lambda copy: copy.wait_send())

    lax.fori_loop(0, blocks, drain, None)


def solution(mesh):
    group = mesh.shape["tp"]
    side = math.isqrt(group)

    def local(x, gain, wq, wk, wv, wo):
        rows, width = x.shape
        inner = wq.shape[1]
        heads = inner // HEAD
        bq = BLOCK
        blocks = rows // bq
        quarter, piece, wide, thin = bq // side, bq // side**2, width // 2, width // 4
        cos, sin = _tables(rows)
        vmem = pl.BlockSpec(memory_space=pltpu.VMEM)
        f32, bf16 = jnp.float32, jnp.bfloat16
        bufs = [pltpu.VMEM((blocks, 2, 2, r, w), bf16) for r, w in ((quarter, thin), (quarter, wide), (piece, thin), (piece, wide))]
        return pl.pallas_call(
            functools.partial(_kernel, side),
            out_shape=jax.ShapeDtypeStruct((rows, width), bf16),
            in_specs=[vmem] * 8,
            out_specs=vmem,
            scratch_shapes=[
                pltpu.VMEM((bq, width), bf16),
                pltpu.VMEM((bq, inner), bf16),
                pltpu.VMEM((rows, inner), bf16),
                pltpu.VMEM((inner, rows), bf16),
                pltpu.VMEM((bq, inner), bf16),
                pltpu.VMEM((heads, bq), f32),
                pltpu.VMEM((heads, 8, bq), f32),
                pltpu.VMEM((heads, HEAD, bq), f32),
                pltpu.VMEM((bq, width), f32),
                pltpu.VMEM((2, quarter, wide), f32),
                *bufs, *bufs,
                pltpu.SemaphoreType.DMA((blocks, 2, 8, 2)),
                pltpu.SemaphoreType.DMA((blocks, 2, 8, 2)),
            ],
            compiler_params=pltpu.CompilerParams(
                vmem_limit_bytes=VMEM, collective_id=0, has_side_effects=True),
        )(x, gain[None], cos, sin, wq, wk, wv, wo)

    tokens, columns = P("dp", None), P(None, "tp")
    return jax.shard_map(
        local,
        mesh=mesh,
        in_specs=(tokens, P(None), columns, columns, columns, P("tp", None)),
        out_specs=tokens,
        check_vma=False,
    )
```

```python
import functools
import math

import jax
import jax.numpy as jnp
import numpy as np
from jax import lax
from jax.experimental import pallas as pl
from jax.experimental.pallas import tpu as pltpu
from jax.sharding import PartitionSpec as P

HEAD = 128
THETA = 10000
LOG2E = 1.4426950408889634
EXP = HEAD**-0.5 * LOG2E
BLOCK = 512
VMEM = 63 * 2**20


def _dot(a, b, ca, cb):
    return lax.dot_general(a, b, (((ca,), (cb,)), ((), ())), preferred_element_type=jnp.float32)


def _tables(rows):
    half = HEAD // 2
    power = (np.float32(THETA) ** (-np.arange(half, dtype=np.float32) / np.float32(half))).astype(np.float32)
    angle = (np.arange(rows, dtype=np.float32)[:, None] * power).astype(np.float64)
    cos, sin = np.cos(angle).astype(np.float32), np.sin(angle).astype(np.float32)
    return np.concatenate([cos, sin], 1)


def _kernel(side, x_hbm, gain_hbm, turn_hbm, wq_hbm, wk_hbm, wv_hbm, wo_hbm, y_ref,
            x_ref, gain_ref, turn_ref, wq_ref, wk_ref, wv_ref, wo_ref, load_sem, a_s, q_s, k_s, vt_s, o_s, top_s, sum_s, mix_s, term_s, part_s,
            out_s, sum2_s, in1, in2, send_sem, recv_sem):
    rows, width = x_ref.shape
    bq = a_s.shape[0]
    blocks = rows // bq
    heads = wq_ref.shape[1] // HEAD
    quarter, piece = bq // side, bq // side**2
    wide = width // 2

    first_rows, other_rows = pl.ds(0, bq), pl.ds(bq, rows - bq)
    early = [(x_hbm.at[first_rows], x_ref.at[first_rows]), (gain_hbm, gain_ref), (turn_hbm.at[first_rows], turn_ref.at[first_rows]),
             (wq_hbm, wq_ref), (wk_hbm, wk_ref), (wv_hbm, wv_ref)]
    late = [(wo_hbm, wo_ref), (x_hbm.at[other_rows], x_ref.at[other_rows]), (turn_hbm.at[other_rows], turn_ref.at[other_rows])]
    loads = [pltpu.make_async_copy(src, dst, load_sem.at[n]) for n, (src, dst) in enumerate(early + late)]
    for load in loads:
        load.start()

    me = lax.axis_index("tp")
    here = (lax.div(me, side), lax.rem(me, side))

    def at(axis, n):
        moved = lax.rem(here[axis] + n + side, side)
        return moved * side + here[1] if axis == 0 else here[0] * side + moved

    others = [[at(axis, n) for n in range(1, side)] for axis in (0, 1)]
    barrier = pltpu.get_barrier_semaphore()
    for line in others:
        for device in line:
            pl.semaphore_signal(barrier, inc=1, device_id={"tp": device}, device_id_type=pl.DeviceIdType.MESH)
    pl.semaphore_wait(barrier, 2 * (side - 1))
    for load in loads[: len(early)]:
        load.wait()


    def step(c, n, action):
        for half in (0, 1):
            first, second = half, 1 - half
            p1, p2 = here[first], here[second]
            cols = pl.ds(half * wide, wide)

            def rows1(k):
                return pl.multiple_of(lax.rem(p1 + k, side) * quarter, quarter)

            def rows2(k):
                return pl.multiple_of(lax.rem(p2 + k, side) * piece, piece)

            for k in range(1, side):
                if n == 0:
                    src, dst = out_s.at[c, pl.ds(rows1(k), quarter), cols], in1.at[c, half, k - 1]
                elif n == 1:
                    src, dst = sum2_s.at[c, half, pl.ds(rows2(k), piece)], in2.at[c, half, k - 1]
                elif n == 2:
                    src = dst = y_ref.at[pl.ds(pl.multiple_of(c * bq + rows1(0) + rows2(0), piece), piece), cols]
                else:
                    src = dst = y_ref.at[pl.ds(pl.multiple_of(c * bq + rows1(0), quarter), quarter), cols]
                action(pltpu.make_async_remote_copy(
                    src_ref=src, dst_ref=dst, send_sem=send_sem.at[c, half, n, k - 1], recv_sem=recv_sem.at[c, half, n, k - 1],
                    device_id={"tp": others[first if n in (0, 3) else second][k - 1]}, device_id_type=pl.DeviceIdType.MESH))

    def prepare(c, n):
        for half in (0, 1):
            p1, p2 = here[half], here[1 - half]
            lo = half * wide
            mine = pl.multiple_of(p1 * quarter, quarter)
            own = pl.multiple_of(p2 * piece, piece)
            if n == 1:
                total = term_s[pl.ds(mine, quarter), lo : lo + wide]
                for k in range(side - 1):
                    total = total + in1[c, half, k].astype(jnp.float32)
                part_s[half] = total
                sum2_s[c, half] = total.astype(jnp.bfloat16)
            elif n == 2:
                total = part_s[half, pl.ds(own, piece), :]
                for k in range(side - 1):
                    total = total + in2[c, half, k].astype(jnp.float32)
                where = pl.ds(pl.multiple_of(c * bq + mine + own, piece), piece)
                y_ref[where, lo : lo + wide] = (x_ref[where, lo : lo + wide].astype(jnp.float32) + total).astype(jnp.bfloat16)

    def advance(c, n):
        @pl.when((c >= 0) & (c < blocks))
        def _():
            if n > 0:
                step(c, n - 1, lambda copy: copy.wait_recv())
            prepare(c, n)
            step(c, n, lambda copy: copy.start())


    def project(i):
        mine = pl.ds(pl.multiple_of(i * bq, bq), bq)
        xw = x_ref[mine, :].astype(jnp.float32)
        scale = lax.rsqrt(jnp.mean(xw * xw, -1, keepdims=True) + 1e-6)
        a_s[...] = (xw * scale * gain_ref[...].astype(jnp.float32)).astype(jnp.bfloat16)
        half = HEAD // 2
        cos, sin = turn_ref[mine, :half], turn_ref[mine, half:]
        cos, sin = jnp.concatenate([cos, cos], 1), jnp.concatenate([-sin, sin], 1)

        def turned(t):
            t = t.astype(jnp.bfloat16).astype(jnp.float32)
            return (t * cos + pltpu.roll(t, half, 1) * sin).astype(jnp.bfloat16)

        two = 2 * HEAD
        for at_ in range(0, heads * HEAD, two):
            q = _dot(a_s[...], wq_ref[:, at_ : at_ + two], 1, 0)
            k = _dot(a_s[...], wk_ref[:, at_ : at_ + two], 1, 0)
            v = _dot(a_s[...], wv_ref[:, at_ : at_ + two], 1, 0)
            for b in (0, HEAD):
                q_s[:, at_ + b : at_ + b + HEAD] = turned(q[:, b : b + HEAD])
                k_s[mine, at_ + b : at_ + b + HEAD] = turned(k[:, b : b + HEAD])
            vt_s[at_ : at_ + two, mine] = v.astype(jnp.bfloat16).T
        top_s[...] = jnp.full(top_s.shape, -jnp.inf, jnp.float32)
        sum_s[...] = jnp.zeros(sum_s.shape, jnp.float32)
        mix_s[...] = jnp.zeros(mix_s.shape, jnp.float32)

    def tile(j, masked):
        keys = pl.ds(pl.multiple_of(j * bq, bq), bq)
        scores, weights, keeps = {}, {}, {}
        if masked:
            ok = lax.broadcasted_iota(jnp.int32, (bq, bq), 1) >= lax.broadcasted_iota(jnp.int32, (bq, bq), 0)

        def score(h):
            cols = slice(h * HEAD, (h + 1) * HEAD)
            scores[h] = _dot(k_s[keys, cols], q_s[:, cols], 1, 1)

        def weigh(h):
            s = jnp.where(ok, scores.pop(h), -jnp.inf) if masked else scores.pop(h)
            old = top_s[h : h + 1, :]
            top = jnp.maximum(old, s.max(axis=0, keepdims=True))
            w = jnp.exp2((s - top) * EXP)
            keep = jnp.exp2((old - top) * EXP)
            top_s[h : h + 1, :] = top
            sum_s[h] = sum_s[h] * keep + w.reshape(bq // 8, 8, bq).sum(axis=0)
            weights[h], keeps[h] = w.astype(jnp.bfloat16), keep

        def mix(h):
            mix_s[h] = mix_s[h] * keeps.pop(h) + _dot(vt_s[h * HEAD : (h + 1) * HEAD, keys], weights.pop(h), 1, 0)

        score(0)
        for h in range(heads):
            if h + 1 < heads:
                score(h + 1)
            weigh(h)
            if h > 0:
                mix(h - 1)
        mix(heads - 1)

    def finish(i):
        for h in range(heads):
            total = sum_s[h].sum(axis=0, keepdims=True)
            o_s[:, h * HEAD : (h + 1) * HEAD] = (mix_s[h] * (1 / total)).astype(jnp.bfloat16).T
        for n in range(0, width, 2 * HEAD):
            term = _dot(o_s[...], wo_ref[:, n : n + 2 * HEAD], 1, 0)
            term_s[:, n : n + 2 * HEAD] = term
            out_s[i, :, n : n + 2 * HEAD] = term.astype(jnp.bfloat16)

    def block(i, _):
        @pl.when(i < blocks)
        def _():
            project(i)

        @pl.when(i == 0)
        def _():
            for load in loads[len(early) :]:
                load.wait()

        whole = lax.select(i < blocks, i, 0)

        @pl.when(whole > 0)
        def _():
            tile(0, False)

        advance(i - 2, 3)
        advance(i - 1, 1)
        lax.fori_loop(1, whole, lambda j, _: tile(j, False), None)

        @pl.when(i < blocks)
        def _():
            tile(i, True)
            finish(i)

        advance(i - 1, 2)
        advance(i, 0)

    lax.fori_loop(0, blocks + 2, block, None)

    def drain(c, _):
        step(c, 3, lambda copy: copy.wait_recv())
        for n in range(4):
            step(c, n, lambda copy: copy.wait_send())

    lax.fori_loop(0, blocks, drain, None)


def solution(mesh):
    group = mesh.shape["tp"]
    side = math.isqrt(group)

    def local(x, gain, wq, wk, wv, wo):
        rows, width = x.shape
        inner = wq.shape[1]
        heads = inner // HEAD
        bq = BLOCK
        blocks = rows // bq
        quarter, piece, wide = bq // side, bq // side**2, width // 2
        vmem = pl.BlockSpec(memory_space=pltpu.VMEM)
        f32, bf16 = jnp.float32, jnp.bfloat16
        return pl.pallas_call(
            functools.partial(_kernel, side),
            out_shape=jax.ShapeDtypeStruct((rows, width), bf16),
            in_specs=[pl.BlockSpec(memory_space=pl.ANY)] * 7,
            out_specs=vmem,
            scratch_shapes=[
                pltpu.VMEM((rows, width), bf16),
                pltpu.VMEM((width,), bf16),
                pltpu.VMEM((rows, HEAD), f32),
                *[pltpu.VMEM((width, inner), bf16)] * 3,
                pltpu.VMEM((inner, width), bf16),
                pltpu.SemaphoreType.DMA((9,)),
                pltpu.VMEM((bq, width), bf16),
                pltpu.VMEM((bq, inner), bf16),
                pltpu.VMEM((rows, inner), bf16),
                pltpu.VMEM((inner, rows), bf16),
                pltpu.VMEM((bq, inner), bf16),
                pltpu.VMEM((heads, bq), f32),
                pltpu.VMEM((heads, 8, bq), f32),
                pltpu.VMEM((heads, HEAD, bq), f32),
                pltpu.VMEM((bq, width), f32),
                pltpu.VMEM((2, quarter, wide), f32),
                pltpu.VMEM((blocks, bq, width), bf16),
                pltpu.VMEM((blocks, 2, quarter, wide), bf16),
                pltpu.VMEM((blocks, 2, side - 1, quarter, wide), bf16),
                pltpu.VMEM((blocks, 2, side - 1, piece, wide), bf16),
                pltpu.SemaphoreType.DMA((blocks, 2, 4, side - 1)),
                pltpu.SemaphoreType.DMA((blocks, 2, 4, side - 1)),
            ],
            compiler_params=pltpu.CompilerParams(
                vmem_limit_bytes=VMEM, collective_id=0, has_side_effects=True),
        )(x, gain, _tables(rows), wq, wk, wv, wo)

    tokens, columns = P("dp", None), P(None, "tp")
    return jax.shard_map(
        local,
        mesh=mesh,
        in_specs=(tokens, P(None), columns, columns, columns, P("tp", None)),
        out_specs=tokens,
        check_vma=False,
    )
```

```python
import functools
import math

import jax
import jax.numpy as jnp
import numpy as np
from jax import lax
from jax.experimental import pallas as pl
from jax.experimental.pallas import tpu as pltpu
from jax.sharding import PartitionSpec as P

HEAD = 128
THETA = 10000
LOG2E = 1.4426950408889634
EXP = HEAD**-0.5 * LOG2E
BLOCK = 512
PARTS = 2
STRIP = 256
VMEM = 57 * 2**20


def _dot(a, b, ca, cb):
    return lax.dot_general(a, b, (((ca,), (cb,)), ((), ())), preferred_element_type=jnp.float32)


def _tables(rows):
    half = HEAD // 2
    power = (np.float32(THETA) ** (-np.arange(half, dtype=np.float32) / np.float32(half))).astype(np.float32)
    angle = (np.arange(rows, dtype=np.float32)[:, None] * power).astype(np.float64)
    cos, sin = np.cos(angle).astype(np.float32), np.sin(angle).astype(np.float32)
    return np.concatenate([cos, sin], 1)


def _kernel(side, x_hbm, gain_hbm, turn_hbm, wq_hbm, wk_hbm, wv_hbm, wo_hbm, y_ref,
            x_ref, gain_ref, turn_ref, wq_ref, wk_ref, wv_ref, wo_ref, load_sem, a_s, q_s, k_s, vt_s, o_s, top_s, sum_s, mix_s, term_s, part_s,
            out_s, sum2_s, in1, in2, send_sem, recv_sem, last_sem):
    rows, width = x_ref.shape
    bq = a_s.shape[0]
    blocks = rows // bq
    cb = bq // PARTS
    chunks = rows // cb
    heads = wq_ref.shape[1] // HEAD
    quarter, piece = cb // side, cb // side**2
    wide = width // 2

    first_rows, other_rows = pl.ds(0, bq), pl.ds(bq, rows - bq)
    early = [(x_hbm.at[first_rows], x_ref.at[first_rows]), (gain_hbm, gain_ref), (turn_hbm.at[first_rows], turn_ref.at[first_rows]),
             (wq_hbm, wq_ref), (wk_hbm, wk_ref), (wv_hbm, wv_ref)]
    late = [(wo_hbm, wo_ref), (x_hbm.at[other_rows], x_ref.at[other_rows]), (turn_hbm.at[other_rows], turn_ref.at[other_rows])]
    loads = [pltpu.make_async_copy(src, dst, load_sem.at[n]) for n, (src, dst) in enumerate(early + late)]
    for load in loads:
        load.start()

    me = lax.axis_index("tp")
    here = (lax.div(me, side), lax.rem(me, side))

    def at(axis, n):
        moved = lax.rem(here[axis] + n + side, side)
        return moved * side + here[1] if axis == 0 else here[0] * side + moved

    others = [[at(axis, n) for n in range(1, side)] for axis in (0, 1)]
    barrier = pltpu.get_barrier_semaphore()
    for line in others:
        for device in line:
            pl.semaphore_signal(barrier, inc=1, device_id={"tp": device}, device_id_type=pl.DeviceIdType.MESH)
    pl.semaphore_wait(barrier, 2 * (side - 1))
    for load in loads[: len(early)]:
        load.wait()


    def arrived(c, n):
        whole = (in1, in2, in2)[n].at[c]
        pltpu.make_async_copy(whole, whole, recv_sem.at[c, n]).wait()

    def send(c, n):
        for half in (0, 1):
            first, second = half, 1 - half
            p1, p2 = here[first], here[second]
            cols = pl.ds(half * wide, wide)

            def rows1(k):
                return pl.multiple_of(lax.rem(p1 + k, side) * quarter, quarter)

            def rows2(k):
                return pl.multiple_of(lax.rem(p2 + k, side) * piece, piece)

            for k in range(1, side):
                if n == 0:
                    src, dst = out_s.at[c, pl.ds(rows1(k), quarter), cols], in1.at[c, half, k - 1]
                elif n == 1:
                    src, dst = sum2_s.at[c, half, pl.ds(rows2(k), piece)], in2.at[c, half, k - 1]
                elif n == 2:
                    src = dst = y_ref.at[pl.ds(pl.multiple_of(c * cb + rows1(0) + rows2(0), piece), piece), cols]
                else:
                    src = dst = y_ref.at[pl.ds(pl.multiple_of(c * cb + rows1(0), quarter), quarter), cols]
                pltpu.make_async_remote_copy(
                    src_ref=src, dst_ref=dst, send_sem=send_sem.at[n // 2], recv_sem=recv_sem.at[c, n] if n < 3 else last_sem,
                    device_id={"tp": others[first if n in (0, 3) else second][k - 1]}, device_id_type=pl.DeviceIdType.MESH).start()

    def prepare(c, n):
        even = lax.rem(c, PARTS)
        for half in (0, 1):
            p1, p2 = here[half], here[1 - half]
            lo = half * wide
            mine = pl.multiple_of(p1 * quarter, quarter)
            own = pl.multiple_of(p2 * piece, piece)
            if n == 1:
                total = term_s[pl.ds(pl.multiple_of(even * cb + mine, quarter), quarter), lo : lo + wide]
                for k in range(side - 1):
                    total = total + in1[c, half, k].astype(jnp.float32)
                part_s[even, half] = total
                sum2_s[c, half] = total.astype(jnp.bfloat16)
            elif n == 2:
                total = part_s[even, half, pl.ds(own, piece), :]
                for k in range(side - 1):
                    total = total + in2[c, half, k].astype(jnp.float32)
                where = pl.ds(pl.multiple_of(c * cb + mine + own, piece), piece)
                y_ref[where, lo : lo + wide] = (x_ref[where, lo : lo + wide].astype(jnp.float32) + total).astype(jnp.bfloat16)

    def advance(c, n):
        @pl.when((c >= 0) & (c < chunks))
        def _():
            if n > 0:
                arrived(c, n - 1)
            prepare(c, n)
            send(c, n)


    def project(i):
        mine = pl.ds(pl.multiple_of(i * bq, bq), bq)
        xw = x_ref[mine, :].astype(jnp.float32)
        scale = lax.rsqrt(jnp.mean(xw * xw, -1, keepdims=True) + 1e-6)
        a_s[...] = (xw * scale * gain_ref[...].astype(jnp.float32)).astype(jnp.bfloat16)
        half = HEAD // 2
        cos, sin = turn_ref[mine, :half], turn_ref[mine, half:]
        cos, sin = jnp.concatenate([cos, cos], 1), jnp.concatenate([-sin, sin], 1)

        def turned(t):
            t = t.astype(jnp.bfloat16).astype(jnp.float32)
            return (t * cos + pltpu.roll(t, half, 1) * sin).astype(jnp.bfloat16)

        two = 2 * HEAD
        for at_ in range(0, heads * HEAD, two):
            q = _dot(a_s[...], wq_ref[:, at_ : at_ + two], 1, 0)
            k = _dot(a_s[...], wk_ref[:, at_ : at_ + two], 1, 0)
            v = _dot(a_s[...], wv_ref[:, at_ : at_ + two], 1, 0)
            for b in (0, HEAD):
                q_s[:, at_ + b : at_ + b + HEAD] = turned(q[:, b : b + HEAD])
                k_s[mine, at_ + b : at_ + b + HEAD] = turned(k[:, b : b + HEAD])
            vt_s[at_ : at_ + two, mine] = v.astype(jnp.bfloat16).T
        top_s[...] = jnp.full(top_s.shape, -jnp.inf, jnp.float32)
        sum_s[...] = jnp.zeros(sum_s.shape, jnp.float32)
        mix_s[...] = jnp.zeros(mix_s.shape, jnp.float32)

    def tile(start, bk, lo, masked):
        keys = pl.ds(pl.multiple_of(start, bk), bk)
        strip = min(STRIP, bq - lo)
        strips = [(h, at_) for h in range(heads) for at_ in range(lo, bq, strip)]
        scores, weights, keeps = {}, {}, {}
        if masked:
            gap = lax.broadcasted_iota(jnp.int32, (bk, strip), 1) - lax.broadcasted_iota(jnp.int32, (bk, strip), 0)

        def score(n):
            h, at_ = strips[n]
            cols = slice(h * HEAD, (h + 1) * HEAD)
            scores[n] = _dot(k_s[keys, cols], q_s[at_ : at_ + strip, cols], 1, 1)

        def weigh(n):
            h, at_ = strips[n]
            here = slice(at_, at_ + strip)
            s = jnp.where(gap >= lo - at_, scores.pop(n), -jnp.inf) if masked else scores.pop(n)
            old = top_s[h : h + 1, here]
            top = jnp.maximum(old, s.max(axis=0, keepdims=True))
            w = jnp.exp2((s - top) * EXP)
            keep = jnp.exp2((old - top) * EXP)
            top_s[h : h + 1, here] = top
            sum_s[h, :, here] = sum_s[h, :, here] * keep + w.reshape(bk // 8, 8, strip).sum(axis=0)
            weights[n], keeps[n] = w.astype(jnp.bfloat16), keep

        def mix(n):
            h, at_ = strips[n]
            here = slice(at_, at_ + strip)
            mix_s[h, :, here] = mix_s[h, :, here] * keeps.pop(n) + _dot(vt_s[h * HEAD : (h + 1) * HEAD, keys], weights.pop(n), 1, 0)

        count, ahead = len(strips), 2
        for n in range(-ahead, count + ahead):
            if 0 <= n + ahead < count:
                score(n + ahead)
            if 0 <= n < count:
                weigh(n)
            if 0 <= n - ahead < count:
                mix(n - ahead)

    def finish(i):
        for h in range(heads):
            total = sum_s[h].sum(axis=0, keepdims=True)
            o_s[:, h * HEAD : (h + 1) * HEAD] = (mix_s[h] * (1 / total)).astype(jnp.bfloat16).T
        for part in range(PARTS):
            for n in range(0, width, 2 * HEAD):
                term = _dot(o_s[part * cb : (part + 1) * cb, :], wo_ref[:, n : n + 2 * HEAD], 1, 0)
                term_s[part * cb : (part + 1) * cb, n : n + 2 * HEAD] = term
                out_s[PARTS * i + part, :, n : n + 2 * HEAD] = term.astype(jnp.bfloat16)
            send(PARTS * i + part, 0)

    late_on = blocks - 1

    def forward(i, n):
        for part in range(PARTS):
            advance(PARTS * i + part, n)

    def block(i, _):
        busy, closing = i < blocks, i >= late_on

        @pl.when(busy)
        def _():
            project(i)

        @pl.when(i == 0)
        def _():
            for load in loads[len(early) :]:
                load.wait()

        @pl.when(i <= late_on)
        def _():
            forward(i - 2, 3)

        whole = lax.select(busy, i, 0)
        soon = jnp.minimum(whole, 1)
        lax.fori_loop(0, soon, lambda j, _: tile(j * bq, bq, 0, False), None)
        forward(i - 1, 1)
        lax.fori_loop(soon, whole, lambda j, _: tile(j * bq, bq, 0, False), None)

        @pl.when(closing)
        def _():
            forward(i - 1, 2)

        @pl.when(busy)
        def _():
            tile(i * bq, bq // 2, 0, True)
            tile(i * bq + bq // 2, bq // 2, bq // 2, True)

        @pl.when(closing)
        def _():
            forward(i - 1, 3)

        @pl.when(jnp.logical_not(closing))
        def _():
            forward(i - 1, 2)

        @pl.when(busy)
        def _():
            finish(i)

    lax.fori_loop(0, blocks + 1, block, None)

    pltpu.make_async_copy(in1, in1, last_sem).wait()
    sent = y_ref.at[pl.ds(0, chunks * 2 * (side - 1) * (quarter + piece) // 2)]
    for n in (0, 1):
        pltpu.make_async_copy(sent, sent, send_sem.at[n]).wait()


def solution(mesh):
    group = mesh.shape["tp"]
    side = math.isqrt(group)

    def local(x, gain, wq, wk, wv, wo):
        rows, width = x.shape
        inner = wq.shape[1]
        heads = inner // HEAD
        bq = BLOCK
        cb = bq // PARTS
        chunks = rows // cb
        quarter, piece, wide = cb // side, cb // side**2, width // 2
        vmem = pl.BlockSpec(memory_space=pltpu.VMEM)
        f32, bf16 = jnp.float32, jnp.bfloat16
        return pl.pallas_call(
            functools.partial(_kernel, side),
            out_shape=pltpu.VMEM((rows, width), bf16),
            in_specs=[pl.BlockSpec(memory_space=pl.ANY)] * 7,
            out_specs=vmem,
            scratch_shapes=[
                pltpu.VMEM((rows, width), bf16),
                pltpu.VMEM((width,), bf16),
                pltpu.VMEM((rows, HEAD), f32),
                *[pltpu.VMEM((width, inner), bf16)] * 3,
                pltpu.VMEM((inner, width), bf16),
                pltpu.SemaphoreType.DMA((9,)),
                pltpu.VMEM((bq, width), bf16),
                pltpu.VMEM((bq, inner), bf16),
                pltpu.VMEM((rows, inner), bf16),
                pltpu.VMEM((inner, rows), bf16),
                pltpu.VMEM((bq, inner), bf16),
                pltpu.VMEM((heads, bq), f32),
                pltpu.VMEM((heads, 8, bq), f32),
                pltpu.VMEM((heads, HEAD, bq), f32),
                pltpu.VMEM((bq, width), f32),
                pltpu.VMEM((PARTS, 2, quarter, wide), f32),
                pltpu.VMEM((chunks, cb, width), bf16),
                pltpu.VMEM((chunks, 2, quarter, wide), bf16),
                pltpu.VMEM((chunks, 2, side - 1, quarter, wide), bf16),
                pltpu.VMEM((chunks, 2, side - 1, piece, wide), bf16),
                pltpu.SemaphoreType.DMA((2,)),
                pltpu.SemaphoreType.DMA((chunks, 3)),
                pltpu.SemaphoreType.DMA,
            ],
            compiler_params=pltpu.CompilerParams(
                vmem_limit_bytes=VMEM, collective_id=0, has_side_effects=True),
        )(x, gain, _tables(rows), wq, wk, wv, wo)

    tokens, columns = P("dp", None), P(None, "tp")
    return jax.shard_map(
        local,
        mesh=mesh,
        in_specs=(tokens, P(None), columns, columns, columns, P("tp", None)),
        out_specs=tokens,
        check_vma=False,
    )
```

```python
import functools
import math

import jax
import jax.numpy as jnp
import numpy as np
from jax import lax
from jax.experimental import pallas as pl
from jax.experimental.pallas import tpu as pltpu
from jax.sharding import PartitionSpec as P

HEAD = 128
THETA = 10000
LOG2E = 1.4426950408889634
EXP = HEAD**-0.5 * LOG2E
BLOCK = 512
PARTS = 2
STRIP = 256
VMEM = 57 * 2**20


def _dot(a, b, ca, cb):
    return lax.dot_general(a, b, (((ca,), (cb,)), ((), ())), preferred_element_type=jnp.float32)


def _tables(rows):
    half = HEAD // 2
    power = (np.float32(THETA) ** (-np.arange(half, dtype=np.float32) / np.float32(half))).astype(np.float32)
    angle = (np.arange(rows, dtype=np.float32)[:, None] * power).astype(np.float64)
    cos, sin = np.cos(angle).astype(np.float32), np.sin(angle).astype(np.float32)
    return np.concatenate([cos, sin], 1)


def _kernel(side, x_hbm, gain_hbm, turn_hbm, wq_hbm, wk_hbm, wv_hbm, wo_hbm, y_ref,
            x_ref, gain_ref, turn_ref, wq_ref, wk_ref, wv_ref, wo_ref, load_sem, a_s, q_s, k_s, vt_s, o_s, top_s, sum_s, mix_s, term_s, part_s,
            out_s, sum2_s, in1, in2, send_sem, recv_sem, last_sem):
    rows, width = x_ref.shape
    bq = a_s.shape[0]
    blocks = rows // bq
    cb = bq // PARTS
    chunks = rows // cb
    heads = wq_ref.shape[1] // HEAD
    quarter, piece = cb // side, cb // side**2
    wide = width // 2

    first_rows, other_rows = pl.ds(0, bq), pl.ds(bq, rows - bq)
    early = [(x_hbm.at[first_rows], x_ref.at[first_rows]), (gain_hbm, gain_ref), (turn_hbm.at[first_rows], turn_ref.at[first_rows]),
             (wq_hbm, wq_ref), (wk_hbm, wk_ref), (wv_hbm, wv_ref)]
    late = [(wo_hbm, wo_ref), (x_hbm.at[other_rows], x_ref.at[other_rows]), (turn_hbm.at[other_rows], turn_ref.at[other_rows])]
    loads = [pltpu.make_async_copy(src, dst, load_sem.at[n]) for n, (src, dst) in enumerate(early + late)]
    for load in loads[: len(early)]:
        load.start()

    me = lax.axis_index("tp")
    here = (lax.div(me, side), lax.rem(me, side))

    def at(axis, n):
        moved = lax.rem(here[axis] + n + side, side)
        return moved * side + here[1] if axis == 0 else here[0] * side + moved

    others = [[at(axis, n) for n in range(1, side)] for axis in (0, 1)]
    barrier = pltpu.get_barrier_semaphore()
    for line in others:
        for device in line:
            pl.semaphore_signal(barrier, inc=1, device_id={"tp": device}, device_id_type=pl.DeviceIdType.MESH)
    pl.semaphore_wait(barrier, 2 * (side - 1))
    for load in loads[: len(early)]:
        load.wait()
    for load in loads[len(early) :]:
        load.start()


    def arrived(c, n):
        whole = (in1, in2, in2)[n].at[c]
        pltpu.make_async_copy(whole, whole, recv_sem.at[c, n]).wait()

    def send(c, n):
        for half in (0, 1):
            first, second = half, 1 - half
            p1, p2 = here[first], here[second]
            cols = pl.ds(half * wide, wide)

            def rows1(k):
                return pl.multiple_of(lax.rem(p1 + k, side) * quarter, quarter)

            def rows2(k):
                return pl.multiple_of(lax.rem(p2 + k, side) * piece, piece)

            for k in range(1, side):
                if n == 0:
                    src, dst = out_s.at[c, pl.ds(rows1(k), quarter), cols], in1.at[c, half, k - 1]
                elif n == 1:
                    src, dst = sum2_s.at[c, half, pl.ds(rows2(k), piece)], in2.at[c, half, k - 1]
                elif n == 2:
                    src = dst = y_ref.at[pl.ds(pl.multiple_of(c * cb + rows1(0) + rows2(0), piece), piece), cols]
                else:
                    src = dst = y_ref.at[pl.ds(pl.multiple_of(c * cb + rows1(0), quarter), quarter), cols]
                pltpu.make_async_remote_copy(
                    src_ref=src, dst_ref=dst, send_sem=send_sem.at[n // 2], recv_sem=recv_sem.at[c, n] if n < 3 else last_sem,
                    device_id={"tp": others[first if n in (0, 3) else second][k - 1]}, device_id_type=pl.DeviceIdType.MESH).start()

    def prepare(c, n):
        even = lax.rem(c, PARTS)
        for half in (0, 1):
            p1, p2 = here[half], here[1 - half]
            lo = half * wide
            mine = pl.multiple_of(p1 * quarter, quarter)
            own = pl.multiple_of(p2 * piece, piece)
            if n == 1:
                total = term_s[pl.ds(pl.multiple_of(even * cb + mine, quarter), quarter), lo : lo + wide]
                for k in range(side - 1):
                    total = total + in1[c, half, k].astype(jnp.float32)
                part_s[even, half] = total
                sum2_s[c, half] = total.astype(jnp.bfloat16)
            elif n == 2:
                total = part_s[even, half, pl.ds(own, piece), :]
                for k in range(side - 1):
                    total = total + in2[c, half, k].astype(jnp.float32)
                where = pl.ds(pl.multiple_of(c * cb + mine + own, piece), piece)
                y_ref[where, lo : lo + wide] = (x_ref[where, lo : lo + wide].astype(jnp.float32) + total).astype(jnp.bfloat16)

    def advance(c, n):
        @pl.when((c >= 0) & (c < chunks))
        def _():
            if n > 0:
                arrived(c, n - 1)
            prepare(c, n)
            send(c, n)


    def project(i):
        mine = pl.ds(pl.multiple_of(i * bq, bq), bq)
        xw = x_ref[mine, :].astype(jnp.float32)
        scale = lax.rsqrt(jnp.mean(xw * xw, -1, keepdims=True) + 1e-6)
        a_s[...] = (xw * scale * gain_ref[...].astype(jnp.float32)).astype(jnp.bfloat16)
        half = HEAD // 2
        cos, sin = turn_ref[mine, :half], turn_ref[mine, half:]
        cos, sin = jnp.concatenate([cos, cos], 1), jnp.concatenate([-sin, sin], 1)

        def turned(t):
            t = t.astype(jnp.bfloat16).astype(jnp.float32)
            return (t * cos + pltpu.roll(t, half, 1) * sin).astype(jnp.bfloat16)

        two = 2 * HEAD
        for at_ in range(0, heads * HEAD, two):
            q = _dot(a_s[...], wq_ref[:, at_ : at_ + two], 1, 0)
            k = _dot(a_s[...], wk_ref[:, at_ : at_ + two], 1, 0)
            v = _dot(a_s[...], wv_ref[:, at_ : at_ + two], 1, 0)
            for b in (0, HEAD):
                q_s[:, at_ + b : at_ + b + HEAD] = turned(q[:, b : b + HEAD])
                k_s[mine, at_ + b : at_ + b + HEAD] = turned(k[:, b : b + HEAD])
            vt_s[at_ : at_ + two, mine] = v.astype(jnp.bfloat16).T
        top_s[...] = jnp.full(top_s.shape, -jnp.inf, jnp.float32)
        sum_s[...] = jnp.zeros(sum_s.shape, jnp.float32)
        mix_s[...] = jnp.zeros(mix_s.shape, jnp.float32)

    def tile(start, bk, lo, masked):
        keys = pl.ds(pl.multiple_of(start, bk), bk)
        strip = min(STRIP, bq - lo)
        strips = [(h, at_) for h in range(heads) for at_ in range(lo, bq, strip)]
        scores, weights, keeps = {}, {}, {}
        if masked:
            gap = lax.broadcasted_iota(jnp.int32, (bk, strip), 1) - lax.broadcasted_iota(jnp.int32, (bk, strip), 0)

        def score(n):
            h, at_ = strips[n]
            cols = slice(h * HEAD, (h + 1) * HEAD)
            scores[n] = _dot(k_s[keys, cols], q_s[at_ : at_ + strip, cols], 1, 1)

        def weigh(n):
            h, at_ = strips[n]
            here = slice(at_, at_ + strip)
            s = jnp.where(gap >= lo - at_, scores.pop(n), -jnp.inf) if masked else scores.pop(n)
            old = top_s[h : h + 1, here]
            top = jnp.maximum(old, s.max(axis=0, keepdims=True))
            w = jnp.exp2((s - top) * EXP)
            keep = jnp.exp2((old - top) * EXP)
            top_s[h : h + 1, here] = top
            sum_s[h, :, here] = sum_s[h, :, here] * keep + w.reshape(bk // 8, 8, strip).sum(axis=0)
            weights[n], keeps[n] = w.astype(jnp.bfloat16), keep

        def mix(n):
            h, at_ = strips[n]
            here = slice(at_, at_ + strip)
            mix_s[h, :, here] = mix_s[h, :, here] * keeps.pop(n) + _dot(vt_s[h * HEAD : (h + 1) * HEAD, keys], weights.pop(n), 1, 0)

        count, ahead = len(strips), 2
        for n in range(-ahead, count + ahead):
            if 0 <= n + ahead < count:
                score(n + ahead)
            if 0 <= n < count:
                weigh(n)
            if 0 <= n - ahead < count:
                mix(n - ahead)

    def finish(i):
        for h in range(heads):
            total = sum_s[h].sum(axis=0, keepdims=True)
            o_s[:, h * HEAD : (h + 1) * HEAD] = (mix_s[h] * (1 / total)).astype(jnp.bfloat16).T
        for part in range(PARTS):
            for n in range(0, width, 2 * HEAD):
                term = _dot(o_s[part * cb : (part + 1) * cb, :], wo_ref[:, n : n + 2 * HEAD], 1, 0)
                term_s[part * cb : (part + 1) * cb, n : n + 2 * HEAD] = term
                out_s[PARTS * i + part, :, n : n + 2 * HEAD] = term.astype(jnp.bfloat16)
            send(PARTS * i + part, 0)

    late_on = blocks - 1

    def forward(i, n):
        for part in range(PARTS):
            advance(PARTS * i + part, n)

    def block(i, _):
        busy, closing = i < blocks, i >= late_on

        @pl.when(busy)
        def _():
            project(i)

        @pl.when(i == 0)
        def _():
            for load in loads[len(early) :]:
                load.wait()

        @pl.when(i <= late_on)
        def _():
            forward(i - 2, 2)

        whole = lax.select(busy, i, 0)
        soon = jnp.minimum(whole, 2)
        lax.fori_loop(0, soon, lambda j, _: tile(j * bq, bq, 0, False), None)

        @pl.when(closing)
        def _():
            forward(i - 1, 1)

        @pl.when(i <= late_on)
        def _():
            forward(i - 2, 3)

        lax.fori_loop(soon, whole, lambda j, _: tile(j * bq, bq, 0, False), None)

        @pl.when(busy)
        def _():
            tile(i * bq, bq // 2, 0, True)
            tile(i * bq + bq // 2, bq // 2, bq // 2, True)

        @pl.when(closing)
        def _():
            forward(i - 1, 2)

        @pl.when(jnp.logical_not(closing))
        def _():
            forward(i - 1, 1)

        @pl.when(busy)
        def _():
            finish(i)

        @pl.when(i > late_on)
        def _():
            forward(i - 2, 3)
            forward(i - 1, 3)

    lax.fori_loop(0, blocks + 1, block, None)

    pltpu.make_async_copy(in1, in1, last_sem).wait()
    sent = y_ref.at[pl.ds(0, chunks * 2 * (side - 1) * (quarter + piece) // 2)]
    for n in (0, 1):
        pltpu.make_async_copy(sent, sent, send_sem.at[n]).wait()


def solution(mesh):
    group = mesh.shape["tp"]
    side = math.isqrt(group)

    def local(x, gain, wq, wk, wv, wo):
        rows, width = x.shape
        inner = wq.shape[1]
        heads = inner // HEAD
        bq = BLOCK
        cb = bq // PARTS
        chunks = rows // cb
        quarter, piece, wide = cb // side, cb // side**2, width // 2
        vmem = pl.BlockSpec(memory_space=pltpu.VMEM)
        f32, bf16 = jnp.float32, jnp.bfloat16
        return pl.pallas_call(
            functools.partial(_kernel, side),
            out_shape=pltpu.VMEM((rows, width), bf16),
            in_specs=[pl.BlockSpec(memory_space=pl.ANY)] * 7,
            out_specs=vmem,
            scratch_shapes=[
                pltpu.VMEM((rows, width), bf16),
                pltpu.VMEM((width,), bf16),
                pltpu.VMEM((rows, HEAD), f32),
                *[pltpu.VMEM((width, inner), bf16)] * 3,
                pltpu.VMEM((inner, width), bf16),
                pltpu.SemaphoreType.DMA((9,)),
                pltpu.VMEM((bq, width), bf16),
                pltpu.VMEM((bq, inner), bf16),
                pltpu.VMEM((rows, inner), bf16),
                pltpu.VMEM((inner, rows), bf16),
                pltpu.VMEM((bq, inner), bf16),
                pltpu.VMEM((heads, bq), f32),
                pltpu.VMEM((heads, 8, bq), f32),
                pltpu.VMEM((heads, HEAD, bq), f32),
                pltpu.VMEM((bq, width), f32),
                pltpu.VMEM((PARTS, 2, quarter, wide), f32),
                pltpu.VMEM((chunks, cb, width), bf16),
                pltpu.VMEM((chunks, 2, quarter, wide), bf16),
                pltpu.VMEM((chunks, 2, side - 1, quarter, wide), bf16),
                pltpu.VMEM((chunks, 2, side - 1, piece, wide), bf16),
                pltpu.SemaphoreType.DMA((2,)),
                pltpu.SemaphoreType.DMA((chunks, 3)),
                pltpu.SemaphoreType.DMA,
            ],
            compiler_params=pltpu.CompilerParams(
                vmem_limit_bytes=VMEM, collective_id=0, has_side_effects=True),
        )(x, gain, _tables(rows), wq, wk, wv, wo)

    tokens, columns = P("dp", None), P(None, "tp")
    return jax.shard_map(
        local,
        mesh=mesh,
        in_specs=(tokens, P(None), columns, columns, columns, P("tp", None)),
        out_specs=tokens,
        check_vma=False,
    )
```

```python
import functools
import math

import jax
import jax.numpy as jnp
import numpy as np
from jax import lax
from jax.experimental import pallas as pl
from jax.experimental.pallas import tpu as pltpu
from jax.sharding import PartitionSpec as P

HEAD = 128
THETA = 10000
LOG2E = 1.4426950408889634
EXP = HEAD**-0.5 * LOG2E
BLOCK = 512
PARTS = 2
STRIP = 256
VMEM = 57 * 2**20


def _dot(a, b, ca, cb):
    return lax.dot_general(a, b, (((ca,), (cb,)), ((), ())), preferred_element_type=jnp.float32)


def _tables(rows):
    half = HEAD // 2
    power = (np.float32(THETA) ** (-np.arange(half, dtype=np.float32) / np.float32(half))).astype(np.float32)
    angle = (np.arange(rows, dtype=np.float32)[:, None] * power).astype(np.float64)
    cos, sin = np.cos(angle).astype(np.float32), np.sin(angle).astype(np.float32)
    return np.concatenate([cos, sin], 1)


def _kernel(side, x_hbm, gain_hbm, turn_hbm, wq_hbm, wk_hbm, wv_hbm, wo_hbm, y_ref,
            x_ref, gain_ref, turn_ref, wq_ref, wk_ref, wv_ref, wo_ref, load_sem, a_s, q_s, k_s, vt_s, o_s, top_s, sum_s, mix_s, term_s, part_s,
            out_s, sum2_s, in1, in2, send_sem, recv_sem, last_sem):
    rows, width = x_ref.shape
    bq = a_s.shape[0]
    blocks = rows // bq
    cb = bq // PARTS
    chunks = rows // cb
    heads = wq_ref.shape[1] // HEAD
    quarter, piece = cb // side, cb // side**2
    wide = width // 2

    first_rows, other_rows = pl.ds(0, bq), pl.ds(bq, rows - bq)
    early = [(x_hbm.at[first_rows], x_ref.at[first_rows]), (gain_hbm, gain_ref), (turn_hbm.at[first_rows], turn_ref.at[first_rows]),
             (wq_hbm, wq_ref), (wk_hbm, wk_ref), (wv_hbm, wv_ref)]
    late = [(wo_hbm, wo_ref), (x_hbm.at[other_rows], x_ref.at[other_rows]), (turn_hbm.at[other_rows], turn_ref.at[other_rows])]
    loads = [pltpu.make_async_copy(src, dst, load_sem.at[n]) for n, (src, dst) in enumerate(early + late)]
    for load in loads[: len(early)]:
        load.start()

    me = lax.axis_index("tp")
    here = (lax.div(me, side), lax.rem(me, side))

    def at(axis, n):
        moved = lax.rem(here[axis] + n + side, side)
        return moved * side + here[1] if axis == 0 else here[0] * side + moved

    others = [[at(axis, n) for n in range(1, side)] for axis in (0, 1)]
    barrier = pltpu.get_barrier_semaphore()
    for line in others:
        for device in line:
            pl.semaphore_signal(barrier, inc=1, device_id={"tp": device}, device_id_type=pl.DeviceIdType.MESH)
    pl.semaphore_wait(barrier, 2 * (side - 1))
    for load in loads[: len(early)]:
        load.wait()
    for load in loads[len(early) :]:
        load.start()


    def arrived(c, n):
        whole = (in1, in2, in2)[n].at[c]
        pltpu.make_async_copy(whole, whole, recv_sem.at[c, n]).wait()

    def send(c, n):
        for half in (0, 1):
            first, second = half, 1 - half
            p1, p2 = here[first], here[second]
            cols = pl.ds(half * wide, wide)

            def rows1(k):
                return pl.multiple_of(lax.rem(p1 + k, side) * quarter, quarter)

            def rows2(k):
                return pl.multiple_of(lax.rem(p2 + k, side) * piece, piece)

            for k in range(1, side):
                if n == 0:
                    src, dst = out_s.at[c, pl.ds(rows1(k), quarter), cols], in1.at[c, half, k - 1]
                elif n == 1:
                    src, dst = sum2_s.at[c, half, pl.ds(rows2(k), piece)], in2.at[c, half, k - 1]
                elif n == 2:
                    src = dst = y_ref.at[pl.ds(pl.multiple_of(c * cb + rows1(0) + rows2(0), piece), piece), cols]
                else:
                    src = dst = y_ref.at[pl.ds(pl.multiple_of(c * cb + rows1(0), quarter), quarter), cols]
                pltpu.make_async_remote_copy(
                    src_ref=src, dst_ref=dst, send_sem=send_sem.at[n // 2], recv_sem=recv_sem.at[c, n] if n < 3 else last_sem,
                    device_id={"tp": others[first if n in (0, 3) else second][k - 1]}, device_id_type=pl.DeviceIdType.MESH).start()

    def prepare(c, n):
        even = lax.rem(c, PARTS)
        for half in (0, 1):
            p1, p2 = here[half], here[1 - half]
            lo = half * wide
            mine = pl.multiple_of(p1 * quarter, quarter)
            own = pl.multiple_of(p2 * piece, piece)
            if n == 1:
                total = term_s[pl.ds(pl.multiple_of(even * cb + mine, quarter), quarter), lo : lo + wide]
                for k in range(side - 1):
                    total = total + in1[c, half, k].astype(jnp.float32)
                part_s[even, half] = total
                sum2_s[c, half] = total.astype(jnp.bfloat16)
            elif n == 2:
                total = part_s[even, half, pl.ds(own, piece), :]
                for k in range(side - 1):
                    total = total + in2[c, half, k].astype(jnp.float32)
                where = pl.ds(pl.multiple_of(c * cb + mine + own, piece), piece)
                y_ref[where, lo : lo + wide] = (x_ref[where, lo : lo + wide].astype(jnp.float32) + total).astype(jnp.bfloat16)

    def advance(c, n):
        @pl.when((c >= 0) & (c < chunks))
        def _():
            if n > 0:
                arrived(c, n - 1)
            prepare(c, n)
            send(c, n)


    def project(i):
        mine = pl.ds(pl.multiple_of(i * bq, bq), bq)
        xw = x_ref[mine, :].astype(jnp.float32)
        scale = lax.rsqrt(jnp.mean(xw * xw, -1, keepdims=True) + 1e-6)
        a_s[...] = (xw * scale * gain_ref[...].astype(jnp.float32)).astype(jnp.bfloat16)
        half = HEAD // 2
        cos, sin = turn_ref[mine, :half], turn_ref[mine, half:]
        cos, sin = jnp.concatenate([cos, cos], 1), jnp.concatenate([-sin, sin], 1)

        def turned(t):
            t = t.astype(jnp.bfloat16).astype(jnp.float32)
            return (t * cos + pltpu.roll(t, half, 1) * sin).astype(jnp.bfloat16)

        two = 2 * HEAD
        for at_ in range(0, heads * HEAD, two):
            q = _dot(a_s[...], wq_ref[:, at_ : at_ + two], 1, 0)
            k = _dot(a_s[...], wk_ref[:, at_ : at_ + two], 1, 0)
            v = _dot(a_s[...], wv_ref[:, at_ : at_ + two], 1, 0)
            for b in (0, HEAD):
                q_s[:, at_ + b : at_ + b + HEAD] = turned(q[:, b : b + HEAD])
                k_s[mine, at_ + b : at_ + b + HEAD] = turned(k[:, b : b + HEAD])
            vt_s[at_ : at_ + two, mine] = v.astype(jnp.bfloat16).T
        top_s[...] = jnp.full(top_s.shape, -jnp.inf, jnp.float32)
        sum_s[...] = jnp.zeros(sum_s.shape, jnp.float32)
        mix_s[...] = jnp.zeros(mix_s.shape, jnp.float32)

    def tile(start, bk, lo, masked):
        keys = pl.ds(pl.multiple_of(start, bk), bk)
        strip = min(STRIP, bq - lo)
        strips = [(h, at_) for h in range(heads) for at_ in range(lo, bq, strip)]
        scores, weights, keeps = {}, {}, {}
        if masked:
            gap = lax.broadcasted_iota(jnp.int32, (bk, strip), 1) - lax.broadcasted_iota(jnp.int32, (bk, strip), 0)

        def score(n):
            h, at_ = strips[n]
            cols = slice(h * HEAD, (h + 1) * HEAD)
            scores[n] = _dot(k_s[keys, cols], q_s[at_ : at_ + strip, cols], 1, 1)

        def weigh(n):
            h, at_ = strips[n]
            here = slice(at_, at_ + strip)
            s = jnp.where(gap >= lo - at_, scores.pop(n), -jnp.inf) if masked else scores.pop(n)
            old = top_s[h : h + 1, here]
            top = jnp.maximum(old, s.max(axis=0, keepdims=True))
            w = jnp.exp2((s - top) * EXP)
            keep = jnp.exp2((old - top) * EXP)
            top_s[h : h + 1, here] = top
            sum_s[h, :, here] = sum_s[h, :, here] * keep + w.reshape(bk // 8, 8, strip).sum(axis=0)
            weights[n], keeps[n] = w.astype(jnp.bfloat16), keep

        def mix(n):
            h, at_ = strips[n]
            here = slice(at_, at_ + strip)
            mix_s[h, :, here] = mix_s[h, :, here] * keeps.pop(n) + _dot(vt_s[h * HEAD : (h + 1) * HEAD, keys], weights.pop(n), 1, 0)

        count, ahead = len(strips), 2
        for n in range(-ahead, count + ahead):
            if 0 <= n + ahead < count:
                score(n + ahead)
            if 0 <= n < count:
                weigh(n)
            if 0 <= n - ahead < count:
                mix(n - ahead)

    def finish(i):
        for h in range(heads):
            total = sum_s[h].sum(axis=0, keepdims=True)
            o_s[:, h * HEAD : (h + 1) * HEAD] = (mix_s[h] * (1 / total)).astype(jnp.bfloat16).T
        for part in range(PARTS):
            for n in range(0, width, 2 * HEAD):
                term = _dot(o_s[part * cb : (part + 1) * cb, :], wo_ref[:, n : n + 2 * HEAD], 1, 0)
                term_s[part * cb : (part + 1) * cb, n : n + 2 * HEAD] = term
                out_s[PARTS * i + part, :, n : n + 2 * HEAD] = term.astype(jnp.bfloat16)
            send(PARTS * i + part, 0)

    late_on = blocks - 1

    def forward(i, n):
        for part in range(PARTS):
            advance(PARTS * i + part, n)

    def block(i, _):
        busy, closing = i < blocks, i >= late_on

        @pl.when(busy)
        def _():
            project(i)

        @pl.when(i == 0)
        def _():
            for load in loads[len(early) :]:
                load.wait()

        @pl.when(i <= late_on)
        def _():
            forward(i - 2, 2)

        whole = lax.select(busy, i, 0)
        soon = jnp.minimum(whole, 2)
        lax.fori_loop(0, soon, lambda j, _: tile(j * bq, bq, 0, False), None)

        @pl.when(closing & busy)
        def _():
            forward(i - 1, 1)

        @pl.when(i <= late_on)
        def _():
            forward(i - 2, 3)

        lax.fori_loop(soon, whole, lambda j, _: tile(j * bq, bq, 0, False), None)

        @pl.when(busy)
        def _():
            tile(i * bq, bq // 2, 0, True)
            tile(i * bq + bq // 2, bq // 2, bq // 2, True)

        @pl.when(closing & busy)
        def _():
            forward(i - 1, 2)

        @pl.when(jnp.logical_not(closing))
        def _():
            forward(i - 1, 1)

        @pl.when(busy)
        def _():
            finish(i)

        @pl.when(i > late_on)
        def _():
            forward(i - 1, 1)
            for part in range(PARTS):
                advance(PARTS * (i - 1) + part, 2)
                advance(PARTS * (i - 2) + part, 3)
            forward(i - 1, 3)

    lax.fori_loop(0, blocks + 1, block, None)

    pltpu.make_async_copy(in1, in1, last_sem).wait()
    sent = y_ref.at[pl.ds(0, chunks * 2 * (side - 1) * (quarter + piece) // 2)]
    for n in (0, 1):
        pltpu.make_async_copy(sent, sent, send_sem.at[n]).wait()


def solution(mesh):
    group = mesh.shape["tp"]
    side = math.isqrt(group)

    def local(x, gain, wq, wk, wv, wo):
        rows, width = x.shape
        inner = wq.shape[1]
        heads = inner // HEAD
        bq = BLOCK
        cb = bq // PARTS
        chunks = rows // cb
        quarter, piece, wide = cb // side, cb // side**2, width // 2
        vmem = pl.BlockSpec(memory_space=pltpu.VMEM)
        f32, bf16 = jnp.float32, jnp.bfloat16
        return pl.pallas_call(
            functools.partial(_kernel, side),
            out_shape=pltpu.VMEM((rows, width), bf16),
            in_specs=[pl.BlockSpec(memory_space=pl.ANY)] * 7,
            out_specs=vmem,
            scratch_shapes=[
                pltpu.VMEM((rows, width), bf16),
                pltpu.VMEM((width,), bf16),
                pltpu.VMEM((rows, HEAD), f32),
                *[pltpu.VMEM((width, inner), bf16)] * 3,
                pltpu.VMEM((inner, width), bf16),
                pltpu.SemaphoreType.DMA((9,)),
                pltpu.VMEM((bq, width), bf16),
                pltpu.VMEM((bq, inner), bf16),
                pltpu.VMEM((rows, inner), bf16),
                pltpu.VMEM((inner, rows), bf16),
                pltpu.VMEM((bq, inner), bf16),
                pltpu.VMEM((heads, bq), f32),
                pltpu.VMEM((heads, 8, bq), f32),
                pltpu.VMEM((heads, HEAD, bq), f32),
                pltpu.VMEM((bq, width), f32),
                pltpu.VMEM((PARTS, 2, quarter, wide), f32),
                pltpu.VMEM((chunks, cb, width), bf16),
                pltpu.VMEM((chunks, 2, quarter, wide), bf16),
                pltpu.VMEM((chunks, 2, side - 1, quarter, wide), bf16),
                pltpu.VMEM((chunks, 2, side - 1, piece, wide), bf16),
                pltpu.SemaphoreType.DMA((2,)),
                pltpu.SemaphoreType.DMA((chunks, 3)),
                pltpu.SemaphoreType.DMA,
            ],
            compiler_params=pltpu.CompilerParams(
                vmem_limit_bytes=VMEM, collective_id=0, has_side_effects=True),
        )(x, gain, _tables(rows), wq, wk, wv, wo)

    tokens, columns = P("dp", None), P(None, "tp")
    return jax.shard_map(
        local,
        mesh=mesh,
        in_specs=(tokens, P(None), columns, columns, columns, P("tp", None)),
        out_specs=tokens,
        check_vma=False,
    )
```
